32 devices in a mesh: group: 2 (over y), hi: 4 (over z), lo: 2 (over x), cuts: 2 (over core).
Axes of the slice: x: 2, y: 2, z: 4, core: 2. Of those that a mesh axis runs over, the one named last changes fastest.
Arguments:
- state_block: float32 [8, 2, 131072], P(('group', 'hi'), 'lo'), parts along dimension 0, may hold values from -6 to 6
- gate_table: float32 [4, 256, 256], replicated, may hold values from -0.375 to 0.375
- closing_table: float32 [4, 2, 2, 256], replicated, may hold values from -1 to 1
- slice_edges: int32 [8, 3], P(('group', 'cuts')), parts along dimension 0, may hold values from 0 to 3
- bit_orders: int32 [2, 8], replicated, may hold values from 0 to 7, each once within a row
Outputs:
- amplitudes: float32 [8, 2, 65536], P(('group', 'hi'), 'lo', 'cuts'), parts along dimension 0
The draws below stay inside these ranges and needn't reach their ends.
There are 2 independent parts, one for each index of `group`. The reference program is written for one: setup_inputs(seed, part) draws one part's arguments, and reference() takes and returns one part's arrays. A program takes and returns all parts, laid end to end along the dimension named above; an argument that names none is the same for every part. Nothing has to cross between parts.
Inputs may be any that keep to these rules, and one draw needn't show every extreme that they name: `bit_orders`: each row is a permutation of 0 to 7.
All inputs are finite; a program needn't handle non-finite values.
Results may differ from the reference program's by a relative error of at most 0.0001.
Values sent between devices are 32-bit elements; how exact they have to be, the bound alone decides.
A program may use at most 64 MiB of HBM per device.

```python
import jax
import jax.numpy as jnp
from jax import lax

BITS = 8
GATE = 256
CLOSED = 2
MIDDLE = 1
EDGES = 4
SLICES = 4
HI_SPAN = 64
LO_SPAN = 128
LOCAL = 131072
AMPS = 65536
N_HI = 4
N_LO = 2


def plant(entries, key, least, high):
    shape = entries.shape
    spot = [jax.random.randint(jax.random.fold_in(key, axis), (), 0, shape[axis]) for axis in range(len(shape))]
    entries = entries.at[tuple(spot)].set(least)
    longest = shape.index(max(shape))
    spot[longest] = (spot[longest] + 1) % shape[longest]
    return entries.at[tuple(spot)].set(high)


def block_levels(stream_key, extent, cuts, low, high):
    loudness = 1.0
    for position, parts in cuts:
        heights = jax.random.uniform(jax.random.fold_in(jax.random.fold_in(stream_key, 6), position), (parts,), jnp.float32, low / len(cuts), high / len(cuts))
        loudness = loudness * jnp.repeat(jnp.exp(heights), extent[position] // parts).reshape((-1,) + (1,) * (len(extent) - 1 - position))
    return loudness


def gaussian(own_key, extent, scale, limit, cuts=(), kind=jnp.bfloat16):
    drawn = scale * jax.random.normal(own_key, extent, jnp.float32)
    if cuts:
        drawn = drawn * block_levels(own_key, extent, cuts, -0.22, 0.18)
    return jnp.clip(drawn, -limit, limit).astype(kind)


def setup_inputs(seed: int = 0, part: int = 0) -> dict:
    splits = jax.random.split(jax.random.key(seed), 6)
    own_keys = jax.random.split(jax.random.fold_in(splits[5], part), 6)
    return {
        "state_block": gaussian(own_keys[0], (N_HI, N_LO, LOCAL), 1.0, 6.0, ((0, 4), (1, 2)), jnp.float32),
        "gate_table": gaussian(splits[1], (EDGES, GATE, GATE), GATE ** -0.5, 0.375, (), jnp.float32),
        "closing_table": jnp.clip(jax.random.uniform(splits[2], (EDGES, 2, CLOSED, GATE), jnp.float32, -1.0, 1.0), -1.0, 1.0),
        "slice_edges": plant(jax.random.randint(own_keys[3], (SLICES, 3), 0, EDGES), jax.random.fold_in(own_keys[3], 1), 0, EDGES - 1).astype(jnp.int32),
        "bit_orders": jax.vmap(lambda own: jax.random.permutation(own, BITS))(jax.random.split(splits[4], 2)).reshape((2, BITS)).astype(jnp.int32),
    }


def permuted(gate, order):
    rows = jnp.arange(GATE, dtype=jnp.int32)
    picked = (rows[:, None] >> order[None, :].astype(jnp.int32)) & 1
    weights = jnp.left_shift(jnp.ones((BITS,), jnp.int32), jnp.arange(BITS, dtype=jnp.int32))
    source = jnp.sum(picked * weights[None, :], axis=1).astype(jnp.int32)
    return jnp.take(gate, source, axis=0)


def reference(state_block, gate_table, closing_table, slice_edges, bit_orders):
    tensor = state_block.reshape(N_HI, N_LO, HI_SPAN, N_HI, CLOSED, MIDDLE, N_LO, LO_SPAN)
    total = jnp.zeros((N_HI, N_LO, AMPS), jnp.float32)
    for slice_index in range(SLICES):
        chosen = slice_edges[slice_index]
        first = permuted(gate_table[chosen[0]], bit_orders[0]).reshape(HI_SPAN, N_HI, HI_SPAN, N_HI)
        second = permuted(gate_table[chosen[1]], bit_orders[1]).reshape(N_LO, LO_SPAN, N_LO, LO_SPAN)
        front = closing_table[chosen[2], 0].reshape(CLOSED, HI_SPAN, N_HI)
        rear = closing_table[chosen[2], 1].reshape(CLOSED, N_LO, LO_SPAN)
        section_one = jnp.einsum('phPH,hlpbzmeq->HlPbzmeq', first, tensor, precision=lax.Precision.HIGHEST)
        weight_one = jnp.transpose(front, (2, 1, 0))
        section_one = section_one * weight_one[:, None, :, None, :, None, None, None]
        section_two = jnp.einsum('lqLQ,hlpbzmeq->hLpbzmeQ', second, section_one, precision=lax.Precision.HIGHEST)
        closed = jnp.einsum('zLQ,hLpbzmeQ->hLpbmeQ', rear, section_two, precision=lax.Precision.HIGHEST)
        total = total + closed.reshape(N_HI, N_LO, AMPS)
    return total
```

```python
import functools

import jax
import jax.numpy as jnp
from jax import lax
from jax.experimental import pallas as pl
from jax.experimental.pallas import tpu as pltpu
from jax.sharding import PartitionSpec as P

BITS = 8
GATE = 256
CLOSED = 2


def permuted(gate, order):
    rows = jnp.arange(GATE, dtype=jnp.int32)
    picked = rows[:, None] >> order[None, :] & 1
    weights = jnp.left_shift(jnp.ones((BITS,), jnp.int32), jnp.arange(BITS, dtype=jnp.int32))
    source = jnp.sum(picked * weights[None, :], axis=1)
    return jnp.take(gate, source, axis=0)


def local_plain(state_block, gate_table, closing_table, slice_edges, bit_orders):
    count_hi = lax.axis_size("hi")
    count_lo = lax.axis_size("lo")
    span_hi = GATE // count_hi
    span_lo = GATE // count_lo
    middle = state_block.shape[2] // (GATE * GATE * CLOSED)
    tensor = state_block.reshape(span_hi, count_hi, CLOSED, middle, count_lo, span_lo)
    turns = slice_edges.shape[0]
    firsts = []
    seconds = []
    fronts = []
    rears = []
    for turn_index in range(turns):
        chosen = slice_edges[turn_index]
        firsts.append(permuted(gate_table[chosen[0]], bit_orders[0]))
        seconds.append(permuted(gate_table[chosen[1]], bit_orders[1]))
        fronts.append(closing_table[chosen[2], 0])
        rears.append(closing_table[chosen[2], 1])
    section_ones = []
    for turn_index in range(turns):

        def apply_first(piece, first=firsts[turn_index], front=fronts[turn_index]):
            shape = piece.shape
            flat = piece.reshape(GATE, -1)
            product = lax.dot_general(
                first,
                flat,
                (((0,), (0,)), ((), ())),
                precision=lax.Precision.HIGHEST,
                preferred_element_type=jnp.float32,
            )
            scaled = jnp.transpose(front).reshape(shape[0], shape[1], shape[2], 1, 1, 1)
            return product.reshape(shape) * scaled

        section_ones.append(
            apply_first(lax.all_to_all(tensor, "hi", split_axis=1, concat_axis=1, tiled=True))
        )
    total = jnp.zeros((span_hi, count_hi, middle, count_lo, span_lo), jnp.float32)
    for turn_index in range(turns):
        current = section_ones[turn_index]

        def apply_second(piece, second=seconds[turn_index], rear=rears[turn_index]):
            shape = piece.shape
            flat = piece.reshape(-1, GATE)
            product = jnp.dot(
                flat, second, precision=lax.Precision.HIGHEST, preferred_element_type=jnp.float32
            )
            product = product.reshape(shape[0], shape[1], shape[2], shape[3], GATE)
            closed = jnp.einsum("phzkg,zg->phkg", product, rear, precision=lax.Precision.HIGHEST)
            return closed.reshape(shape[0], shape[1], shape[3], shape[4], shape[5])

        total = total + apply_second(
            lax.all_to_all(current, "lo", split_axis=4, concat_axis=4, tiled=True)
        )
    placed = lax.all_to_all(
        lax.all_to_all(total, "hi", split_axis=1, concat_axis=1, tiled=True),
        "lo",
        split_axis=3,
        concat_axis=3,
        tiled=True,
    )
    summed = lax.psum_scatter(placed.reshape(-1), "cuts", scatter_dimension=0, tiled=True)
    return summed.reshape(1, 1, -1)


MESH = pl.DeviceIdType.MESH
HALF = jnp.bfloat16
FULL = jnp.float32


def dot(left, right, dims=((1,), (0,))):
    return lax.dot_general(left, right, (dims, ((), ())), preferred_element_type=FULL)


def halves(value):
    high = value.astype(HALF)
    return high, (value - high.astype(FULL)).astype(HALF)


def source_row(index, orders_ref, section):
    total = jnp.zeros_like(index)
    for bit in range(BITS):
        picked = lax.shift_right_logical(index, jnp.full_like(index, orders_ref[section, bit])) & 1
        total = total | (picked << bit)
    return total


def flipped(index, mask):
    bit = 1
    while bit <= mask:
        if mask & bit:
            index = index + bit - 2 * bit * (index // bit % 2)
        bit *= 2
    return index


def kernel(
    count_hi,
    count_lo,
    x_hbm,
    gate_hbm,
    closing_hbm,
    edges_hbm,
    orders_hbm,
    out_ref,
    x_ref,
    gate_ref,
    closing_ref,
    edges_ref,
    orders_ref,
    outgoing,
    arrived,
    edges_far,
    first_ref,
    second_ref,
    sums,
    result,
    landed,
    local_sems,
    edge_sems,
    ready,
    in_send,
    in_recv,
    out_send,
    out_recv,
):
    hi, lo, cut = lax.axis_index("hi"), lax.axis_index("lo"), lax.axis_index("cuts")
    other = 1 - cut
    span_hi, span_lo = GATE // count_hi, GATE // count_lo
    half = count_hi // 2
    upper, inner = hi // half, hi % half
    rows = GATE // 2
    per = span_hi // 2
    blocks = count_hi * count_lo
    turns = edges_ref.shape[0]
    edges = gate_ref.shape[0]
    near = [(a, b) for a in range(half) for b in range(count_lo)]
    pairs = (
        (x_hbm, x_ref),
        (edges_hbm, edges_ref),
        (orders_hbm, orders_ref),
        (closing_hbm, closing_ref),
        (gate_hbm, gate_ref),
    )
    gets = [pltpu.make_async_copy(*pair, local_sems.at[i]) for i, pair in enumerate(pairs)]
    for get in gets:
        get.start()

    def device(side, a, b, core):
        th = flipped(upper, side) * half + flipped(inner, a)
        return {"hi": th, "lo": flipped(lo, b), "cuts": core}

    def block(a, b, core):
        return (flipped(inner, a) * CLOSED + core) * count_lo + flipped(lo, b)

    def greet(semaphore, side):
        for a, b in near:
            for core in range(CLOSED):
                if side or a or b:
                    pl.semaphore_signal(
                        semaphore, inc=1, device_id=device(side, a, b, core), device_id_type=MESH
                    )

    barrier = pltpu.get_barrier_semaphore()
    pl.semaphore_signal(barrier, inc=1, device_id={"cuts": other}, device_id_type=MESH)
    greet(barrier, 0)

    @pl.when(upper == 0)
    def _():
        greet(barrier, 1)

    gets[0].wait()
    stride = count_hi * CLOSED * count_lo
    for b in range(count_hi):
        for e in range(count_lo):
            start = b * CLOSED * count_lo + cut * count_lo + e
            outgoing[b * count_lo + e] = x_ref[pl.ds(start, span_hi, stride=stride), :]
    arrived[0, 0, cut] = outgoing[block(0, 0, cut)]
    pl.semaphore_wait(barrier, blocks - 1 + upper * blocks)

    sends = []
    for core in range(CLOSED):
        for a, b in sorted(near[1:], key=lambda spot: (spot[0] > 0, spot[1] == 0)):
            k = a * count_lo + b
            copy = pltpu.make_async_remote_copy(
                src_ref=outgoing.at[block(a, b, core)],
                dst_ref=arrived.at[a, b, cut],
                send_sem=in_send.at[core, k],
                recv_sem=in_recv.at[cut, k],
                device_id=device(0, a, b, core),
                device_id_type=MESH,
            )
            copy.start()
            sends.append(copy)
    copy = pltpu.make_async_remote_copy(
        src_ref=outgoing.at[block(0, 0, other)],
        dst_ref=arrived.at[0, 0, cut],
        send_sem=in_send.at[0, 0],
        recv_sem=in_recv.at[cut, 0],
        device_id={"cuts": other},
        device_id_type=MESH,
    )
    copy.start()
    sends.append(copy)

    gets[1].wait()
    edge_copy = pltpu.make_async_remote_copy(
        src_ref=edges_ref,
        dst_ref=edges_far,
        send_sem=edge_sems.at[0],
        recv_sem=edge_sems.at[1],
        device_id={"cuts": other},
        device_id_type=MESH,
    )
    edge_copy.start()

    @pl.when(upper == 1)
    def _():
        greet(ready, 1)

    gets[2].wait()
    down = lax.broadcasted_iota(jnp.int32, (GATE, GATE), 0)
    along = lax.broadcasted_iota(jnp.int32, (GATE, GATE), 1)

    def high_bits(side, a):
        return (side ^ upper) * half + (a ^ inner)

    column = down % span_hi * count_hi + high_bits(down // rows, down % rows // span_hi)
    columns = (column == along).astype(FULL).astype(HALF)
    row = down % span_hi * count_hi + high_bits(0, down % rows // span_hi)
    rows_one = (source_row(row[:rows], orders_ref, 0) == along[:rows]).astype(FULL).astype(HALF)
    row = (down // span_lo ^ lo) * span_lo + down % span_lo
    rows_two = (source_row(row, orders_ref, 1) == along).astype(FULL).astype(HALF)

    gets[3].wait()
    gets[4].wait()
    edge_copy.wait()
    wide = CLOSED * span_hi
    rears = []
    for s in range(2 * turns):
        chosen = edges_ref if s < turns else edges_far
        turn = s % turns

        def pick(place, values):
            total = None
            for c in range(edges):
                weight = (chosen[turn : turn + 1, place : place + 1] == c).astype(FULL)
                term = weight * values(c)
                total = term if total is None else total + term
            return total

        rears.append(pick(2, lambda c: closing_ref[c, 1]))
        fronts = pick(2, lambda c: closing_ref[c, 0])
        gate = pick(0, lambda c: gate_ref[c])
        split = [halves(gate * fronts[z : z + 1]) for z in range(CLOSED)]
        for part in range(2):
            moved = [dot(rows_one, split[z][part]).astype(HALF) for z in range(CLOSED)]
            moved = dot(columns, jnp.concatenate(moved, axis=0), ((1,), (1,))).astype(HALF)
            for side in range(2):
                for a in range(half):
                    for z in range(CLOSED):
                        start = z * rows + a * span_hi
                        first_ref[
                            part, a, side, :, s * wide + z * span_hi : s * wide + (z + 1) * span_hi
                        ] = moved[side * rows : (side + 1) * rows, start : start + span_hi]
        for part, piece in enumerate(halves(pick(1, lambda c: gate_ref[c]))):
            second_ref[part, s] = dot(rows_two, piece).astype(HALF)

    def advance(a):
        for b in range(count_lo):
            for core in range(CLOSED) if a or b else (other,):
                pltpu.make_async_remote_copy(
                    src_ref=outgoing.at[0],
                    dst_ref=arrived.at[a, b, core],
                    send_sem=in_send.at[0, 0],
                    recv_sem=in_recv.at[core, a * count_lo + b],
                    device_id={"cuts": other},
                    device_id_type=MESH,
                ).wait_recv()
        piece = jnp.concatenate(
            [arrived[a, b].reshape(wide, span_lo) for b in range(count_lo)], axis=1
        )
        high, low = halves(piece)
        parts = []
        for s in range(2 * turns):
            part = dot(high, second_ref[0, s]) + dot(low, second_ref[0, s]) + dot(high, second_ref[1, s])
            for z in range(CLOSED):
                parts.append(part[z * span_hi : (z + 1) * span_hi] * rears[s][z : z + 1])
        high, low = halves(jnp.concatenate(parts, axis=0))

        def side_sum(side):
            left, rest = first_ref[0, a, side], first_ref[1, a, side]
            return dot(left, high) + dot(left, low) + dot(rest, high)

        return side_sum

    for a in range(half - 1):
        side_sum = advance(a)
        for side in range(2):
            if a == 0:
                sums[side] = side_sum(side)
            else:
                sums[side] += side_sum(side)
    side_sum = advance(half - 1)
    outs = []
    for side in (1, 0):
        total = sums[side] + side_sum(side) if half > 1 else side_sum(side)
        for e in range(count_lo):
            result[side, e] = total[:, e * span_lo : (e + 1) * span_lo]
        if side:

            @pl.when(upper == 0)
            def _():
                pl.semaphore_wait(ready, blocks)

        for a, b in near:
            ra, rb = inner ^ a, lo ^ b
            spot = ra * count_lo + rb
            for core in range(CLOSED):
                copy = pltpu.make_async_remote_copy(
                    src_ref=result.at[
                        side, b, pl.ds(pl.multiple_of(ra * span_hi + core * per, per), per)
                    ],
                    dst_ref=landed.at[side, spot, cut],
                    send_sem=out_send.at[side, a * count_lo + b, core],
                    recv_sem=out_recv.at[side, spot, cut],
                    device_id={"hi": flipped(upper, side) * half + a, "lo": b, "cuts": core},
                    device_id_type=MESH,
                )
                outs.append((side, a, b, core, copy))
                if side:
                    copy.start()
                else:
                    pl.when((spot > 0) | (cut != core))(copy.start)
    for a, b in near:
        k = a * count_lo + b
        for core in range(CLOSED) if a or b else (other, cut):
            for side in range(2):
                if side or a or b or core is other:
                    pltpu.make_async_remote_copy(
                        src_ref=result.at[0, 0, pl.ds(0, per)],
                        dst_ref=landed.at[side, k, core],
                        send_sem=out_send.at[0, 0, 0],
                        recv_sem=out_recv.at[side, k, core],
                        device_id={"cuts": other},
                        device_id_type=MESH,
                    ).wait_recv()
            if a or b or core is other:
                mine = landed[0, k, core]
            else:
                mine = result[0, lo, pl.ds(pl.multiple_of(cut * per, per), per), :]
            out_ref[pl.ds(block(a, b, core), per, stride=blocks), :] = mine + landed[1, k, core]
    for copy in sends:
        copy.wait_send()
    for side, a, b, core, copy in outs:
        if side:
            copy.wait_send()
        else:
            pl.when(((inner ^ a) > 0) | ((lo ^ b) > 0) | (cut != core))(copy.wait_send)


def local(state_block, gate_table, closing_table, slice_edges, bit_orders):
    count_hi = lax.axis_size("hi")
    count_lo = lax.axis_size("lo")
    span_hi = GATE // count_hi
    span_lo = GATE // count_lo
    blocks = count_hi * count_lo
    half = count_hi // 2
    middle = state_block.shape[2] // (GATE * GATE * CLOSED)
    fits = middle == 1 and span_lo == 128 and span_hi % 16 == 0 and count_hi % 2 == 0
    if not fits or lax.axis_size("cuts") != CLOSED:
        return local_plain(state_block, gate_table, closing_table, slice_edges, bit_orders)
    slices = slice_edges.shape[0] * CLOSED
    rows = GATE // 2
    per = span_hi // 2
    hbm = pl.BlockSpec(memory_space=pltpu.HBM)
    dma = pltpu.SemaphoreType.DMA
    out = pl.pallas_call(
        functools.partial(kernel, count_hi, count_lo),
        out_shape=jax.ShapeDtypeStruct((per * blocks, span_lo), FULL),
        in_specs=[hbm] * 5,
        out_specs=pl.BlockSpec(memory_space=pltpu.VMEM),
        scratch_shapes=[
            pltpu.VMEM((span_hi * blocks * CLOSED, span_lo), FULL),
            pltpu.VMEM(gate_table.shape, FULL),
            pltpu.VMEM(closing_table.shape, FULL),
            pltpu.VMEM(slice_edges.shape, jnp.int32),
            pltpu.SMEM(bit_orders.shape, jnp.int32),
            pltpu.VMEM((blocks, span_hi, span_lo), FULL),
            pltpu.VMEM((half, count_lo, CLOSED, span_hi, span_lo), FULL),
            pltpu.VMEM(slice_edges.shape, jnp.int32),
            pltpu.VMEM((2, half, 2, rows, slices * CLOSED * span_hi), HALF),
            pltpu.VMEM((2, slices, GATE, GATE), HALF),
            pltpu.VMEM((2, rows, GATE), FULL),
            pltpu.VMEM((2, count_lo, rows, span_lo), FULL),
            pltpu.VMEM((2, half * count_lo, CLOSED, per, span_lo), FULL),
            dma((5,)),
            dma((2,)),
            pltpu.SemaphoreType.REGULAR,
            dma((CLOSED, half * count_lo)),
            dma((CLOSED, half * count_lo)),
            dma((2, half * count_lo, CLOSED)),
            dma((2, half * count_lo, CLOSED)),
        ],
        compiler_params=pltpu.CompilerParams(
            collective_id=0, has_side_effects=True, vmem_limit_bytes=32 * 1024 * 1024
        ),
    )(
        *(
            pltpu.with_memory_space_constraint(item, pltpu.HBM)
            for item in (
                state_block.reshape(-1, span_lo),
                gate_table,
                closing_table,
                slice_edges,
                bit_orders,
            )
        )
    )
    return out.reshape(1, 1, -1)


def solution(mesh):
    in_specs = (P(("group", "hi"), "lo", None), P(), P(), P(("group", "cuts"), None), P())
    out_specs = P(("group", "hi"), "lo", "cuts")
    return jax.shard_map(local, mesh=mesh, in_specs=in_specs, out_specs=out_specs, check_vma=False)
```

```python
import functools

import jax
import jax.numpy as jnp
from jax import lax
from jax.experimental import pallas as pl
from jax.experimental.pallas import tpu as pltpu
from jax.sharding import PartitionSpec as P

BITS = 8
STEPS = ((1, 0, 3, 2), (3, 2, 0, 1))
ORDERS = ("SWF", "SWF")
GATE = 256
CLOSED = 2


def permuted(gate, order):
    rows = jnp.arange(GATE, dtype=jnp.int32)
    picked = rows[:, None] >> order[None, :] & 1
    weights = jnp.left_shift(jnp.ones((BITS,), jnp.int32), jnp.arange(BITS, dtype=jnp.int32))
    source = jnp.sum(picked * weights[None, :], axis=1)
    return jnp.take(gate, source, axis=0)


def local_plain(state_block, gate_table, closing_table, slice_edges, bit_orders):
    count_hi = lax.axis_size("hi")
    count_lo = lax.axis_size("lo")
    span_hi = GATE // count_hi
    span_lo = GATE // count_lo
    middle = state_block.shape[2] // (GATE * GATE * CLOSED)
    tensor = state_block.reshape(span_hi, count_hi, CLOSED, middle, count_lo, span_lo)
    turns = slice_edges.shape[0]
    firsts = []
    seconds = []
    fronts = []
    rears = []
    for turn_index in range(turns):
        chosen = slice_edges[turn_index]
        firsts.append(permuted(gate_table[chosen[0]], bit_orders[0]))
        seconds.append(permuted(gate_table[chosen[1]], bit_orders[1]))
        fronts.append(closing_table[chosen[2], 0])
        rears.append(closing_table[chosen[2], 1])
    section_ones = []
    for turn_index in range(turns):

        def apply_first(piece, first=firsts[turn_index], front=fronts[turn_index]):
            shape = piece.shape
            flat = piece.reshape(GATE, -1)
            product = lax.dot_general(
                first,
                flat,
                (((0,), (0,)), ((), ())),
                precision=lax.Precision.HIGHEST,
                preferred_element_type=jnp.float32,
            )
            scaled = jnp.transpose(front).reshape(shape[0], shape[1], shape[2], 1, 1, 1)
            return product.reshape(shape) * scaled

        section_ones.append(
            apply_first(lax.all_to_all(tensor, "hi", split_axis=1, concat_axis=1, tiled=True))
        )
    total = jnp.zeros((span_hi, count_hi, middle, count_lo, span_lo), jnp.float32)
    for turn_index in range(turns):
        current = section_ones[turn_index]

        def apply_second(piece, second=seconds[turn_index], rear=rears[turn_index]):
            shape = piece.shape
            flat = piece.reshape(-1, GATE)
            product = jnp.dot(
                flat, second, precision=lax.Precision.HIGHEST, preferred_element_type=jnp.float32
            )
            product = product.reshape(shape[0], shape[1], shape[2], shape[3], GATE)
            closed = jnp.einsum("phzkg,zg->phkg", product, rear, precision=lax.Precision.HIGHEST)
            return closed.reshape(shape[0], shape[1], shape[3], shape[4], shape[5])

        total = total + apply_second(
            lax.all_to_all(current, "lo", split_axis=4, concat_axis=4, tiled=True)
        )
    placed = lax.all_to_all(
        lax.all_to_all(total, "hi", split_axis=1, concat_axis=1, tiled=True),
        "lo",
        split_axis=3,
        concat_axis=3,
        tiled=True,
    )
    summed = lax.psum_scatter(placed.reshape(-1), "cuts", scatter_dimension=0, tiled=True)
    return summed.reshape(1, 1, -1)


MESH = pl.DeviceIdType.MESH
HALF = jnp.bfloat16
FULL = jnp.float32


def dot(left, right, dims=((1,), (0,))):
    return lax.dot_general(left, right, (dims, ((), ())), preferred_element_type=FULL)


def halves(value):
    high = value.astype(HALF)
    return high, (value - high.astype(FULL)).astype(HALF)


def source_row(index, orders_ref, section):
    total = jnp.zeros_like(index)
    for bit in range(BITS):
        picked = lax.shift_right_logical(index, jnp.full_like(index, orders_ref[section, bit])) & 1
        total = total | (picked << bit)
    return total


def flipped(index, mask):
    bit = 1
    while bit <= mask:
        if mask & bit:
            index = index + bit - 2 * bit * (index // bit % 2)
        bit *= 2
    return index


def kernel(
    count_hi,
    count_lo,
    x_hbm,
    gate_hbm,
    closing_hbm,
    edges_hbm,
    orders_hbm,
    out_ref,
    x_ref,
    gate_ref,
    closing_ref,
    edges_ref,
    orders_ref,
    outgoing,
    arrived,
    edges_far,
    first_ref,
    second_ref,
    sums,
    result,
    landed,
    local_sems,
    edge_sems,
    ready,
    in_send,
    in_recv,
    out_send,
    out_recv,
):
    hi, lo, cut = lax.axis_index("hi"), lax.axis_index("lo"), lax.axis_index("cuts")
    other = 1 - cut
    span_hi, span_lo = GATE // count_hi, GATE // count_lo
    half = count_hi // 2
    upper, inner = hi // half, hi % half
    rows = GATE // 2
    per = span_hi // 2
    blocks = count_hi * count_lo
    turns = edges_ref.shape[0]
    edges = gate_ref.shape[0]
    near = [(a, b) for a in range(half) for b in range(count_lo)]
    cores = [(a, b, core) for a, b in near for core in range(CLOSED)]

    def keeper(a, b, core):
        if core == CLOSED - 1 and a == half - 1:
            return 0
        if core == CLOSED - 1 and b == 1:
            return 1
        return None

    def holder(a, core, half_index):
        return a

    def here(a, b, core):
        return (inner == holder(a, core, upper)) & (lo == b) & (cut == core)

    def any_of(half_index):
        return functools.reduce(
            lambda p, q: p | q,
            [here(*spot) for spot in cores if keeper(*spot) == half_index],
            hi < 0,
        )

    kept = [any_of(0), any_of(1)]
    wide_role = (kept[0] & (upper == 0)) | (kept[1] & (upper == 1))
    idle = (kept[0] & (upper == 1)) | (kept[1] & (upper == 0))
    slots = []
    for spot in cores:
        done = sum(keeper(*item) is None for item in cores[: len(slots)])
        slots.append((len(slots), len(cores) + done))
    mine = [0, 0]
    for spot, pair in zip(cores, slots):
        for side in range(2):
            index = pair[side if keeper(*spot) is None else 0]
            mine[side] += here(*spot).astype(jnp.int32) * index
    taken = len(cores) + sum(keeper(*spot) is None for spot in cores)
    pairs = (
        (x_hbm, x_ref),
        (edges_hbm, edges_ref),
        (orders_hbm, orders_ref),
        (closing_hbm, closing_ref),
        (gate_hbm, gate_ref),
    )
    gets = [pltpu.make_async_copy(*pair, local_sems.at[i]) for i, pair in enumerate(pairs)]
    for get in gets:
        get.start()

    def device(side, a, b, core):
        th = flipped(upper, side) * half + flipped(inner, a)
        return {"hi": th, "lo": flipped(lo, b), "cuts": core}

    def greet(semaphore, side):
        for a, b in near:
            for core in range(CLOSED):
                if side or a or b:
                    pl.semaphore_signal(
                        semaphore, inc=1, device_id=device(side, a, b, core), device_id_type=MESH
                    )

    barrier = pltpu.get_barrier_semaphore()
    pl.semaphore_signal(barrier, inc=1, device_id={"cuts": other}, device_id_type=MESH)
    greet(barrier, 0)

    @pl.when((upper == 0) | kept[1])
    def _():
        greet(barrier, 1)

    gets[0].wait()
    stride = count_hi * CLOSED * count_lo
    for b in range(count_hi):
        for e in range(count_lo):
            start = b * CLOSED * count_lo + cut * count_lo + e
            outgoing[b * count_lo + e] = x_ref[pl.ds(start, span_hi, stride=stride), :]
    guests = sum(keeper(*spot) == 1 for spot in cores)
    pl.semaphore_wait(barrier, blocks - 1 + jnp.where(upper == 1, blocks, guests))

    for half_index, order in enumerate(ORDERS):
        for group in order:
            for a, b, core in cores:
                keep = keeper(a, b, core)
                kind = "S" if keep is None else "W" if keep == half_index else "F"
                if kind != group:
                    continue
                goal_half = half_index if keep is None else keep
                goal = holder(a, core, goal_half)
                k = (inner ^ goal) + (half if kind == "F" else 0)
                copy = pltpu.make_async_remote_copy(
                    src_ref=outgoing.at[(a * CLOSED + core) * count_lo + b],
                    dst_ref=arrived.at[k, lo ^ b, cut],
                    send_sem=in_send,
                    recv_sem=in_recv.at[k],
                    device_id={"hi": goal + goal_half * half, "lo": b, "cuts": core},
                    device_id_type=MESH,
                )
                away = upper == half_index
                if kind != "F":
                    away = away & ~here(a, b, core)
                pl.when(away)(copy.start)
    own = holder(inner, cut, upper)
    own_copy = pltpu.make_async_copy(
        outgoing.at[(own * CLOSED + cut) * count_lo + lo], arrived.at[0, 0, cut], in_recv.at[0]
    )
    pl.when(~idle)(own_copy.start)

    gets[1].wait()
    edge_copy = pltpu.make_async_remote_copy(
        src_ref=edges_ref,
        dst_ref=edges_far,
        send_sem=edge_sems.at[0],
        recv_sem=edge_sems.at[1],
        device_id={"cuts": other},
        device_id_type=MESH,
    )
    edge_copy.start()

    @pl.when(upper == 1)
    def _():
        greet(ready, 1)

    gets[2].wait()
    down = lax.broadcasted_iota(jnp.int32, (GATE, GATE), 0)
    along = lax.broadcasted_iota(jnp.int32, (GATE, GATE), 1)

    def high_bits(side, a):
        return (side ^ upper) * half + (a ^ inner)

    column = down % span_hi * count_hi + high_bits(down // rows, down % rows // span_hi)
    columns = (column == along).astype(FULL).astype(HALF)
    rows_one = (source_row(column, orders_ref, 0) == along).astype(FULL).astype(HALF)
    row = (down // span_lo ^ lo) * span_lo + down % span_lo
    rows_two = (source_row(row, orders_ref, 1) == along).astype(FULL).astype(HALF)

    gets[3].wait()
    gets[4].wait()
    edge_copy.wait()
    wide = CLOSED * span_hi

    def pick(s, place, values):
        chosen = edges_ref if s < turns else edges_far
        turn = s % turns
        total = None
        for c in range(edges):
            weight = (chosen[turn : turn + 1, place : place + 1] == c).astype(FULL)
            term = weight * values(c)
            total = term if total is None else total + term
        return total

    def build_first(s, far):
        fronts = pick(s, 2, lambda c: closing_ref[c, 0])
        gate = pick(s, 0, lambda c: gate_ref[c])
        split = [halves(gate * fronts[z : z + 1]) for z in range(CLOSED)]
        chosen_rows = rows_one[far * rows : (far + 1) * rows]
        for part in range(2):
            moved = [dot(chosen_rows, split[z][part]).astype(HALF) for z in range(CLOSED)]
            moved = dot(columns, jnp.concatenate(moved, axis=0), ((1,), (1,))).astype(HALF)
            for side in range(2):
                for a in range(half):
                    for z in range(CLOSED):
                        start = z * rows + a * span_hi
                        first_ref[
                            far * half + a,
                            side,
                            part * rows : (part + 1) * rows,
                            s * wide + z * span_hi : s * wide + (z + 1) * span_hi,
                        ] = moved[side * rows : (side + 1) * rows, start : start + span_hi]

    rears = []
    for s in range(2 * turns):
        rears.append(pick(s, 2, lambda c: closing_ref[c, 1]))
        build_first(s, 0)
        for part, piece in enumerate(halves(pick(s, 1, lambda c: gate_ref[c]))):
            second_ref[part, s] = dot(rows_two, piece).astype(HALF)

    @pl.when(wide_role)
    def _():
        for s in range(2 * turns):
            build_first(s, 1)

    def advance(a):
        pltpu.make_async_copy(arrived.at[a], arrived.at[a], in_recv.at[a]).wait()
        piece = jnp.concatenate(
            [arrived[a, b].reshape(wide, span_lo) for b in range(count_lo)], axis=1
        )
        high, low = halves(piece)
        pair = jnp.concatenate([high, low], axis=0)
        parts = []
        for s in range(2 * turns):
            both = dot(pair, second_ref[0, s])
            part = both[:wide] + both[wide:] + dot(high, second_ref[1, s])
            for z in range(CLOSED):
                parts.append(part[z * span_hi : (z + 1) * span_hi] * rears[s][z : z + 1])
        high, low = halves(jnp.concatenate(parts, axis=0))

        def side_sum(side):
            both = dot(first_ref[a, side], high)
            return both[:rows] + both[rows:] + dot(first_ref[a, side, :rows, :], low)

        return side_sum

    def gather(a, start=False):
        side_sum = advance(a)
        for side in range(2):
            if start:
                sums[side] = side_sum(side)
            else:
                sums[side] += side_sum(side)

    outs = []
    for goal in range(2):
        side = goal ^ upper
        for a, b, core in cores if goal == 0 else sorted(cores, key=lambda spot: -spot[0]):
            source = result.at[
                goal, b, pl.ds(pl.multiple_of((inner ^ a) * span_hi + core * per, per), per)
            ]
            target = landed.at[jnp.where(side == 0, mine[0], mine[1])]
            copy = pltpu.make_async_remote_copy(
                src_ref=source,
                dst_ref=target,
                send_sem=out_send,
                recv_sem=out_recv,
                device_id={"hi": goal * half + a, "lo": b, "cuts": core},
                device_id_type=MESH,
            )
            at_home = (upper == goal) & (inner == a) & (lo == b) & (cut == core)
            outs.append((goal, ~at_home, copy))

    def finish(a):
        side_sum = advance(a)
        for goal in range(2):
            side = goal ^ upper
            total = sums[side] + side_sum(side)
            for e in range(count_lo):
                result[goal, e] = total[:, e * span_lo : (e + 1) * span_lo]
            if goal:

                @pl.when(upper == 0)
                def _():
                    pl.semaphore_wait(ready, blocks)

            for order, away, copy in outs:
                if order == goal:
                    pl.when(away)(copy.start)
        pltpu.make_async_copy(
            result.at[upper, lo, pl.ds(pl.multiple_of((cut * per), per), per)],
            landed.at[mine[0]],
            out_recv,
        ).start()

    @pl.when(~wide_role & ~idle)
    def _():
        for a in range(half - 1):
            gather(a, a == 0)
        finish(half - 1)

    @pl.when(kept[0] & (upper == 0))
    def _():
        for a in STEPS[0][:-1]:
            gather(a, a == STEPS[0][0])
        finish(STEPS[0][-1])

    @pl.when(kept[1] & (upper == 1))
    def _():
        for a in STEPS[1][:-1]:
            gather(a, a == STEPS[1][0])
        finish(STEPS[1][-1])

    @pl.when(idle & (upper == 0))
    def _():
        pl.semaphore_wait(ready, blocks)

    arrivals = landed.at[pl.ds(0, taken)]

    pltpu.make_async_copy(arrivals, arrivals, out_recv).wait()
    for (a, b, core), (first, second) in zip(cores, slots):
        place = pl.ds((a * CLOSED + core) * count_lo + b, per, stride=blocks)
        if keeper(a, b, core) is not None:
            out_ref[place, :] = landed[first]
        else:
            out_ref[place, :] = landed[first] + landed[second]
    gone = outgoing.at[pl.ds(0, blocks - 1)]
    pltpu.make_async_copy(gone, gone, in_send).wait()

    @pl.when(idle)
    def _():
        pltpu.make_async_copy(outgoing.at[0], outgoing.at[0], in_send).wait()

    @pl.when(~idle)
    def _():
        gone = landed.at[pl.ds(0, 2 * blocks - 1)]
        pltpu.make_async_copy(gone, gone, out_send).wait()


def local(state_block, gate_table, closing_table, slice_edges, bit_orders):
    count_hi = lax.axis_size("hi")
    count_lo = lax.axis_size("lo")
    span_hi = GATE // count_hi
    span_lo = GATE // count_lo
    blocks = count_hi * count_lo
    half = count_hi // 2
    middle = state_block.shape[2] // (GATE * GATE * CLOSED)
    fits = middle == 1 and span_lo == 128 and span_hi % 16 == 0 and count_hi % 2 == 0
    if not fits or lax.axis_size("cuts") != CLOSED:
        return local_plain(state_block, gate_table, closing_table, slice_edges, bit_orders)
    slices = slice_edges.shape[0] * CLOSED
    rows = GATE // 2
    per = span_hi // 2
    hbm = pl.BlockSpec(memory_space=pltpu.HBM)
    dma = pltpu.SemaphoreType.DMA
    out = pl.pallas_call(
        functools.partial(kernel, count_hi, count_lo),
        out_shape=jax.ShapeDtypeStruct((per * blocks, span_lo), FULL),
        in_specs=[hbm] * 5,
        out_specs=pl.BlockSpec(memory_space=pltpu.VMEM),
        scratch_shapes=[
            pltpu.VMEM((span_hi * blocks * CLOSED, span_lo), FULL),
            pltpu.VMEM(gate_table.shape, FULL),
            pltpu.VMEM(closing_table.shape, FULL),
            pltpu.VMEM(slice_edges.shape, jnp.int32),
            pltpu.SMEM(bit_orders.shape, jnp.int32),
            pltpu.VMEM((blocks, span_hi, span_lo), FULL),
            pltpu.VMEM((count_hi, count_lo, CLOSED, span_hi, span_lo), FULL),
            pltpu.VMEM(slice_edges.shape, jnp.int32),
            pltpu.VMEM((count_hi, 2, 2 * rows, slices * CLOSED * span_hi), HALF),
            pltpu.VMEM((2, slices, GATE, GATE), HALF),
            pltpu.VMEM((2, rows, GATE), FULL),
            pltpu.VMEM((2, count_lo, rows, span_lo), FULL),
            pltpu.VMEM((2 * blocks, per, span_lo), FULL),
            dma((5,)),
            dma((2,)),
            pltpu.SemaphoreType.REGULAR,
            dma(()),
            dma((count_hi,)),
            dma(()),
            dma(()),
        ],
        compiler_params=pltpu.CompilerParams(
            collective_id=0, has_side_effects=True, vmem_limit_bytes=32 * 1024 * 1024
        ),
    )(
        *(
            pltpu.with_memory_space_constraint(item, pltpu.HBM)
            for item in (
                state_block.reshape(-1, span_lo),
                gate_table,
                closing_table,
                slice_edges,
                bit_orders,
            )
        )
    )
    return out.reshape(1, 1, -1)


def solution(mesh):
    in_specs = (P(("group", "hi"), "lo", None), P(), P(), P(("group", "cuts"), None), P())
    out_specs = P(("group", "hi"), "lo", "cuts")
    return jax.shard_map(local, mesh=mesh, in_specs=in_specs, out_specs=out_specs, check_vma=False)
```

```python
import functools

import jax
import jax.numpy as jnp
from jax import lax
from jax.experimental import pallas as pl
from jax.experimental.pallas import tpu as pltpu
from jax.sharding import PartitionSpec as P

BITS = 8
STEPS = ((3, 0, 1, 2), (3, 0, 2, 1))
ORDERS = ("SWF", "SFW")
GATE = 256
CLOSED = 2


def permuted(gate, order):
    rows = jnp.arange(GATE, dtype=jnp.int32)
    picked = rows[:, None] >> order[None, :] & 1
    weights = jnp.left_shift(jnp.ones((BITS,), jnp.int32), jnp.arange(BITS, dtype=jnp.int32))
    source = jnp.sum(picked * weights[None, :], axis=1)
    return jnp.take(gate, source, axis=0)


def local_plain(state_block, gate_table, closing_table, slice_edges, bit_orders):
    count_hi = lax.axis_size("hi")
    count_lo = lax.axis_size("lo")
    span_hi = GATE // count_hi
    span_lo = GATE // count_lo
    middle = state_block.shape[2] // (GATE * GATE * CLOSED)
    tensor = state_block.reshape(span_hi, count_hi, CLOSED, middle, count_lo, span_lo)
    turns = slice_edges.shape[0]
    firsts = []
    seconds = []
    fronts = []
    rears = []
    for turn_index in range(turns):
        chosen = slice_edges[turn_index]
        firsts.append(permuted(gate_table[chosen[0]], bit_orders[0]))
        seconds.append(permuted(gate_table[chosen[1]], bit_orders[1]))
        fronts.append(closing_table[chosen[2], 0])
        rears.append(closing_table[chosen[2], 1])
    section_ones = []
    for turn_index in range(turns):

        def apply_first(piece, first=firsts[turn_index], front=fronts[turn_index]):
            shape = piece.shape
            flat = piece.reshape(GATE, -1)
            product = lax.dot_general(
                first,
                flat,
                (((0,), (0,)), ((), ())),
                precision=lax.Precision.HIGHEST,
                preferred_element_type=jnp.float32,
            )
            scaled = jnp.transpose(front).reshape(shape[0], shape[1], shape[2], 1, 1, 1)
            return product.reshape(shape) * scaled

        section_ones.append(
            apply_first(lax.all_to_all(tensor, "hi", split_axis=1, concat_axis=1, tiled=True))
        )
    total = jnp.zeros((span_hi, count_hi, middle, count_lo, span_lo), jnp.float32)
    for turn_index in range(turns):
        current = section_ones[turn_index]

        def apply_second(piece, second=seconds[turn_index], rear=rears[turn_index]):
            shape = piece.shape
            flat = piece.reshape(-1, GATE)
            product = jnp.dot(
                flat, second, precision=lax.Precision.HIGHEST, preferred_element_type=jnp.float32
            )
            product = product.reshape(shape[0], shape[1], shape[2], shape[3], GATE)
            closed = jnp.einsum("phzkg,zg->phkg", product, rear, precision=lax.Precision.HIGHEST)
            return closed.reshape(shape[0], shape[1], shape[3], shape[4], shape[5])

        total = total + apply_second(
            lax.all_to_all(current, "lo", split_axis=4, concat_axis=4, tiled=True)
        )
    placed = lax.all_to_all(
        lax.all_to_all(total, "hi", split_axis=1, concat_axis=1, tiled=True),
        "lo",
        split_axis=3,
        concat_axis=3,
        tiled=True,
    )
    summed = lax.psum_scatter(placed.reshape(-1), "cuts", scatter_dimension=0, tiled=True)
    return summed.reshape(1, 1, -1)


MESH = pl.DeviceIdType.MESH
HALF = jnp.bfloat16
FULL = jnp.float32


def dot(left, right, dims=((1,), (0,))):
    return lax.dot_general(left, right, (dims, ((), ())), preferred_element_type=FULL)


def halves(value):
    high = value.astype(HALF)
    return high, (value - high.astype(FULL)).astype(HALF)


def source_row(index, orders_ref, section):
    total = jnp.zeros_like(index)
    for bit in range(BITS):
        picked = lax.shift_right_logical(index, jnp.full_like(index, orders_ref[section, bit])) & 1
        total = total | (picked << bit)
    return total


def flipped(index, mask):
    bit = 1
    while bit <= mask:
        if mask & bit:
            index = index + bit - 2 * bit * (index // bit % 2)
        bit *= 2
    return index


def kernel(
    count_hi,
    count_lo,
    x_hbm,
    gate_hbm,
    closing_hbm,
    edges_hbm,
    orders_hbm,
    out_ref,
    x_ref,
    gate_ref,
    closing_ref,
    edges_ref,
    orders_ref,
    outgoing,
    arrived,
    edges_far,
    first_ref,
    second_ref,
    sums,
    result,
    landed,
    local_sems,
    edge_sems,
    ready,
    in_send,
    in_recv,
    out_send,
    out_recv,
):
    hi, lo, cut = lax.axis_index("hi"), lax.axis_index("lo"), lax.axis_index("cuts")
    other = 1 - cut
    span_hi, span_lo = GATE // count_hi, GATE // count_lo
    half = count_hi // 2
    upper, inner = hi // half, hi % half
    rows = GATE // 2
    per = span_hi // 2
    blocks = count_hi * count_lo
    turns = edges_ref.shape[0]
    edges = gate_ref.shape[0]
    near = [(a, b) for a in range(half) for b in range(count_lo)]
    cores = [(a, b, core) for a, b in near for core in range(CLOSED)]

    def keeper(a, b, core):
        if core == CLOSED - 1 and a == half - 1:
            return 0
        if core == CLOSED - 1 and b == 1:
            return 1
        return None

    def holder(a, core, half_index):
        return a

    def here(a, b, core):
        return (inner == holder(a, core, upper)) & (lo == b) & (cut == core)

    def any_of(half_index):
        return functools.reduce(
            lambda p, q: p | q,
            [here(*spot) for spot in cores if keeper(*spot) == half_index],
            hi < 0,
        )

    kept = [any_of(0), any_of(1)]
    wide_role = (kept[0] & (upper == 0)) | (kept[1] & (upper == 1))
    idle = (kept[0] & (upper == 1)) | (kept[1] & (upper == 0))
    slots = []
    for spot in cores:
        done = sum(keeper(*item) is None for item in cores[: len(slots)])
        slots.append((len(slots), len(cores) + done))
    mine = [0, 0]
    for spot, pair in zip(cores, slots):
        for side in range(2):
            index = pair[side if keeper(*spot) is None else 0]
            mine[side] += here(*spot).astype(jnp.int32) * index
    taken = len(cores) + sum(keeper(*spot) is None for spot in cores)
    pairs = (
        (x_hbm, x_ref),
        (edges_hbm, edges_ref),
        (orders_hbm, orders_ref),
        (closing_hbm, closing_ref),
        (gate_hbm, gate_ref),
    )
    gets = [pltpu.make_async_copy(*pair, local_sems.at[i]) for i, pair in enumerate(pairs)]
    for get in gets:
        get.start()

    def device(side, a, b, core):
        th = flipped(upper, side) * half + flipped(inner, a)
        return {"hi": th, "lo": flipped(lo, b), "cuts": core}

    def greet(semaphore, side):
        for a, b in near:
            for core in range(CLOSED):
                if side or a or b:
                    pl.semaphore_signal(
                        semaphore, inc=1, device_id=device(side, a, b, core), device_id_type=MESH
                    )

    barrier = pltpu.get_barrier_semaphore()
    pl.semaphore_signal(barrier, inc=1, device_id={"cuts": other}, device_id_type=MESH)
    greet(barrier, 0)

    @pl.when((upper == 0) | kept[1])
    def _():
        greet(barrier, 1)

    gets[0].wait()
    stride = count_hi * CLOSED * count_lo
    for b in range(count_hi):
        for e in range(count_lo):
            start = b * CLOSED * count_lo + cut * count_lo + e
            outgoing[b * count_lo + e] = x_ref[pl.ds(start, span_hi, stride=stride), :]
    guests = sum(keeper(*spot) == 1 for spot in cores)
    pl.semaphore_wait(barrier, blocks - 1 + jnp.where(upper == 1, blocks, guests))

    for half_index, order in enumerate(ORDERS):
        for group in order:
            for a, b, core in cores:
                keep = keeper(a, b, core)
                kind = "S" if keep is None else "W" if keep == half_index else "F"
                if kind != group:
                    continue
                goal_half = half_index if keep is None else keep
                goal = holder(a, core, goal_half)
                k = (inner ^ goal) + (half if kind == "F" else 0)
                copy = pltpu.make_async_remote_copy(
                    src_ref=outgoing.at[(a * CLOSED + core) * count_lo + b],
                    dst_ref=arrived.at[k, lo ^ b, cut],
                    send_sem=in_send,
                    recv_sem=in_recv.at[k],
                    device_id={"hi": goal + goal_half * half, "lo": b, "cuts": core},
                    device_id_type=MESH,
                )
                away = upper == half_index
                if kind != "F":
                    away = away & ~here(a, b, core)
                pl.when(away)(copy.start)
    own = holder(inner, cut, upper)
    own_copy = pltpu.make_async_copy(
        outgoing.at[(own * CLOSED + cut) * count_lo + lo], arrived.at[0, 0, cut], in_recv.at[0]
    )
    pl.when(~idle)(own_copy.start)

    gets[1].wait()
    edge_copy = pltpu.make_async_remote_copy(
        src_ref=edges_ref,
        dst_ref=edges_far,
        send_sem=edge_sems.at[0],
        recv_sem=edge_sems.at[1],
        device_id={"cuts": other},
        device_id_type=MESH,
    )
    edge_copy.start()

    @pl.when(upper == 1)
    def _():
        greet(ready, 1)

    gets[2].wait()
    down = lax.broadcasted_iota(jnp.int32, (GATE, GATE), 0)
    along = lax.broadcasted_iota(jnp.int32, (GATE, GATE), 1)

    def high_bits(side, a):
        return (side ^ upper) * half + (a ^ inner)

    column = down % span_hi * count_hi + high_bits(down // rows, down % rows // span_hi)
    columns = (column == along).astype(FULL).astype(HALF)
    rows_one = (source_row(column, orders_ref, 0) == along).astype(FULL).astype(HALF)
    row = (down // span_lo ^ lo) * span_lo + down % span_lo
    rows_two = (source_row(row, orders_ref, 1) == along).astype(FULL).astype(HALF)

    gets[3].wait()
    gets[4].wait()
    edge_copy.wait()
    wide = CLOSED * span_hi

    def pick(s, place, values):
        chosen = edges_ref if s < turns else edges_far
        turn = s % turns
        total = None
        for c in range(edges):
            weight = (chosen[turn : turn + 1, place : place + 1] == c).astype(FULL)
            term = weight * values(c)
            total = term if total is None else total + term
        return total

    def build_first(s, far):
        fronts = pick(s, 2, lambda c: closing_ref[c, 0])
        gate = pick(s, 0, lambda c: gate_ref[c])
        split = [halves(gate * fronts[z : z + 1]) for z in range(CLOSED)]
        chosen_rows = rows_one[far * rows : (far + 1) * rows]
        for part in range(2):
            moved = [dot(chosen_rows, split[z][part]).astype(HALF) for z in range(CLOSED)]
            moved = dot(columns, jnp.concatenate(moved, axis=0), ((1,), (1,))).astype(HALF)
            for side in range(2):
                for a in range(half):
                    for z in range(CLOSED):
                        start = z * rows + a * span_hi
                        first_ref[
                            far * half + a,
                            side,
                            part * rows : (part + 1) * rows,
                            s * wide + z * span_hi : s * wide + (z + 1) * span_hi,
                        ] = moved[side * rows : (side + 1) * rows, start : start + span_hi]

    rears = []
    for s in range(2 * turns):
        rears.append(pick(s, 2, lambda c: closing_ref[c, 1]))
        build_first(s, 0)
        for part, piece in enumerate(halves(pick(s, 1, lambda c: gate_ref[c]))):
            second_ref[part, s] = dot(rows_two, piece).astype(HALF)

    @pl.when(wide_role)
    def _():
        for s in range(2 * turns):
            build_first(s, 1)

    def advance(a):
        pltpu.make_async_copy(arrived.at[a], arrived.at[a], in_recv.at[a]).wait()
        piece = jnp.concatenate(
            [arrived[a, b].reshape(wide, span_lo) for b in range(count_lo)], axis=1
        )
        high, low = halves(piece)
        pair = jnp.concatenate([high, low], axis=0)
        parts = []
        for s in range(2 * turns):
            both = dot(pair, second_ref[0, s])
            part = both[:wide] + both[wide:] + dot(high, second_ref[1, s])
            for z in range(CLOSED):
                parts.append(part[z * span_hi : (z + 1) * span_hi] * rears[s][z : z + 1])
        high, low = halves(jnp.concatenate(parts, axis=0))

        def side_sum(side):
            both = dot(first_ref[a, side], high)
            return both[:rows] + both[rows:] + dot(first_ref[a, side, :rows, :], low)

        return side_sum

    def gather(a, start=False):
        side_sum = advance(a)
        for side in range(2):
            if start:
                sums[side] = side_sum(side)
            else:
                sums[side] += side_sum(side)

    outs = []
    for goal in range(2):
        side = goal ^ upper
        for a, b, core in cores if goal == 0 else sorted(cores, key=lambda spot: (-spot[0], -spot[1])):
            source = result.at[
                goal, b, pl.ds(pl.multiple_of((inner ^ a) * span_hi + core * per, per), per)
            ]
            target = landed.at[jnp.where(side == 0, mine[0], mine[1])]
            copy = pltpu.make_async_remote_copy(
                src_ref=source,
                dst_ref=target,
                send_sem=out_send,
                recv_sem=out_recv,
                device_id={"hi": goal * half + a, "lo": b, "cuts": core},
                device_id_type=MESH,
            )
            at_home = (upper == goal) & (inner == a) & (lo == b) & (cut == core)
            outs.append((goal, ~at_home, copy))

    def finish(a):
        side_sum = advance(a)
        for goal in range(2):
            side = goal ^ upper
            total = sums[side] + side_sum(side)
            for e in range(count_lo):
                result[goal, e] = total[:, e * span_lo : (e + 1) * span_lo]
            if goal:

                @pl.when(upper == 0)
                def _():
                    pl.semaphore_wait(ready, blocks)

            for order, away, copy in outs:
                if order == goal:
                    pl.when(away)(copy.start)
        pltpu.make_async_copy(
            result.at[upper, lo, pl.ds(pl.multiple_of((cut * per), per), per)],
            landed.at[mine[0]],
            out_recv,
        ).start()

    @pl.when(~wide_role & ~idle)
    def _():
        for a in range(half - 1):
            gather(a, a == 0)
        finish(half - 1)

    @pl.when(kept[0] & (upper == 0))
    def _():
        for a in STEPS[0][:-1]:
            gather(a, a == STEPS[0][0])
        finish(STEPS[0][-1])

    @pl.when(kept[1] & (upper == 1))
    def _():
        for a in STEPS[1][:-1]:
            gather(a, a == STEPS[1][0])
        finish(STEPS[1][-1])

    @pl.when(idle & (upper == 0))
    def _():
        pl.semaphore_wait(ready, blocks)

    arrivals = landed.at[pl.ds(0, taken)]

    pltpu.make_async_copy(arrivals, arrivals, out_recv).wait()
    for (a, b, core), (first, second) in zip(cores, slots):
        place = pl.ds((a * CLOSED + core) * count_lo + b, per, stride=blocks)
        if keeper(a, b, core) is not None:
            out_ref[place, :] = landed[first]
        else:
            out_ref[place, :] = landed[first] + landed[second]
    gone = outgoing.at[pl.ds(0, blocks - 1)]
    pltpu.make_async_copy(gone, gone, in_send).wait()

    @pl.when(idle)
    def _():
        pltpu.make_async_copy(outgoing.at[0], outgoing.at[0], in_send).wait()

    @pl.when(~idle)
    def _():
        gone = landed.at[pl.ds(0, 2 * blocks - 1)]
        pltpu.make_async_copy(gone, gone, out_send).wait()


def local(state_block, gate_table, closing_table, slice_edges, bit_orders):
    count_hi = lax.axis_size("hi")
    count_lo = lax.axis_size("lo")
    span_hi = GATE // count_hi
    span_lo = GATE // count_lo
    blocks = count_hi * count_lo
    half = count_hi // 2
    middle = state_block.shape[2] // (GATE * GATE * CLOSED)
    fits = middle == 1 and span_lo == 128 and span_hi % 16 == 0 and count_hi % 2 == 0
    if not fits or lax.axis_size("cuts") != CLOSED:
        return local_plain(state_block, gate_table, closing_table, slice_edges, bit_orders)
    slices = slice_edges.shape[0] * CLOSED
    rows = GATE // 2
    per = span_hi // 2
    hbm = pl.BlockSpec(memory_space=pltpu.HBM)
    dma = pltpu.SemaphoreType.DMA
    out = pl.pallas_call(
        functools.partial(kernel, count_hi, count_lo),
        out_shape=jax.ShapeDtypeStruct((per * blocks, span_lo), FULL),
        in_specs=[hbm] * 5,
        out_specs=pl.BlockSpec(memory_space=pltpu.VMEM),
        scratch_shapes=[
            pltpu.VMEM((span_hi * blocks * CLOSED, span_lo), FULL),
            pltpu.VMEM(gate_table.shape, FULL),
            pltpu.VMEM(closing_table.shape, FULL),
            pltpu.VMEM(slice_edges.shape, jnp.int32),
            pltpu.SMEM(bit_orders.shape, jnp.int32),
            pltpu.VMEM((blocks, span_hi, span_lo), FULL),
            pltpu.VMEM((count_hi, count_lo, CLOSED, span_hi, span_lo), FULL),
            pltpu.VMEM(slice_edges.shape, jnp.int32),
            pltpu.VMEM((count_hi, 2, 2 * rows, slices * CLOSED * span_hi), HALF),
            pltpu.VMEM((2, slices, GATE, GATE), HALF),
            pltpu.VMEM((2, rows, GATE), FULL),
            pltpu.VMEM((2, count_lo, rows, span_lo), FULL),
            pltpu.VMEM((2 * blocks, per, span_lo), FULL),
            dma((5,)),
            dma((2,)),
            pltpu.SemaphoreType.REGULAR,
            dma(()),
            dma((count_hi,)),
            dma(()),
            dma(()),
        ],
        compiler_params=pltpu.CompilerParams(
            collective_id=0, has_side_effects=True, vmem_limit_bytes=32 * 1024 * 1024
        ),
    )(
        *(
            pltpu.with_memory_space_constraint(item, pltpu.HBM)
            for item in (
                state_block.reshape(-1, span_lo),
                gate_table,
                closing_table,
                slice_edges,
                bit_orders,
            )
        )
    )
    return out.reshape(1, 1, -1)


def solution(mesh):
    in_specs = (P(("group", "hi"), "lo", None), P(), P(), P(("group", "cuts"), None), P())
    out_specs = P(("group", "hi"), "lo", "cuts")
    return jax.shard_map(local, mesh=mesh, in_specs=in_specs, out_specs=out_specs, check_vma=False)
```

```python
import functools

import jax
import jax.numpy as jnp
from jax import lax
from jax.experimental import pallas as pl
from jax.experimental.pallas import tpu as pltpu
from jax.sharding import PartitionSpec as P

BITS = 8
STEPS = ((3, 0, 1, 2), (3, 0, 2, 1))
ORDERS = ("SWF", "SFW")
GATE = 256
CLOSED = 2


def permuted(gate, order):
    rows = jnp.arange(GATE, dtype=jnp.int32)
    picked = rows[:, None] >> order[None, :] & 1
    weights = jnp.left_shift(jnp.ones((BITS,), jnp.int32), jnp.arange(BITS, dtype=jnp.int32))
    source = jnp.sum(picked * weights[None, :], axis=1)
    return jnp.take(gate, source, axis=0)


def local_plain(state_block, gate_table, closing_table, slice_edges, bit_orders):
    count_hi = lax.axis_size("hi")
    count_lo = lax.axis_size("lo")
    span_hi = GATE // count_hi
    span_lo = GATE // count_lo
    middle = state_block.shape[2] // (GATE * GATE * CLOSED)
    tensor = state_block.reshape(span_hi, count_hi, CLOSED, middle, count_lo, span_lo)
    turns = slice_edges.shape[0]
    firsts = []
    seconds = []
    fronts = []
    rears = []
    for turn_index in range(turns):
        chosen = slice_edges[turn_index]
        firsts.append(permuted(gate_table[chosen[0]], bit_orders[0]))
        seconds.append(permuted(gate_table[chosen[1]], bit_orders[1]))
        fronts.append(closing_table[chosen[2], 0])
        rears.append(closing_table[chosen[2], 1])
    section_ones = []
    for turn_index in range(turns):

        def apply_first(piece, first=firsts[turn_index], front=fronts[turn_index]):
            shape = piece.shape
            flat = piece.reshape(GATE, -1)
            product = lax.dot_general(
                first,
                flat,
                (((0,), (0,)), ((), ())),
                precision=lax.Precision.HIGHEST,
                preferred_element_type=jnp.float32,
            )
            scaled = jnp.transpose(front).reshape(shape[0], shape[1], shape[2], 1, 1, 1)
            return product.reshape(shape) * scaled

        section_ones.append(
            apply_first(lax.all_to_all(tensor, "hi", split_axis=1, concat_axis=1, tiled=True))
        )
    total = jnp.zeros((span_hi, count_hi, middle, count_lo, span_lo), jnp.float32)
    for turn_index in range(turns):
        current = section_ones[turn_index]

        def apply_second(piece, second=seconds[turn_index], rear=rears[turn_index]):
            shape = piece.shape
            flat = piece.reshape(-1, GATE)
            product = jnp.dot(
                flat, second, precision=lax.Precision.HIGHEST, preferred_element_type=jnp.float32
            )
            product = product.reshape(shape[0], shape[1], shape[2], shape[3], GATE)
            closed = jnp.einsum("phzkg,zg->phkg", product, rear, precision=lax.Precision.HIGHEST)
            return closed.reshape(shape[0], shape[1], shape[3], shape[4], shape[5])

        total = total + apply_second(
            lax.all_to_all(current, "lo", split_axis=4, concat_axis=4, tiled=True)
        )
    placed = lax.all_to_all(
        lax.all_to_all(total, "hi", split_axis=1, concat_axis=1, tiled=True),
        "lo",
        split_axis=3,
        concat_axis=3,
        tiled=True,
    )
    summed = lax.psum_scatter(placed.reshape(-1), "cuts", scatter_dimension=0, tiled=True)
    return summed.reshape(1, 1, -1)


MESH = pl.DeviceIdType.MESH
HALF = jnp.bfloat16
FULL = jnp.float32


def dot(left, right, dims=((1,), (0,))):
    return lax.dot_general(left, right, (dims, ((), ())), preferred_element_type=FULL)


def halves(value):
    high = value.astype(HALF)
    return high, (value - high.astype(FULL)).astype(HALF)


def source_row(index, orders_ref, section):
    total = jnp.zeros_like(index)
    for bit in range(BITS):
        picked = lax.shift_right_logical(index, jnp.full_like(index, orders_ref[section, bit])) & 1
        total = total | (picked << bit)
    return total


def flipped(index, mask):
    bit = 1
    while bit <= mask:
        if mask & bit:
            index = index + bit - 2 * bit * (index // bit % 2)
        bit *= 2
    return index


def kernel(
    count_hi,
    count_lo,
    x_hbm,
    gate_hbm,
    closing_hbm,
    edges_hbm,
    orders_hbm,
    out_ref,
    x_ref,
    gate_ref,
    closing_ref,
    edges_ref,
    orders_ref,
    outgoing,
    arrived,
    edges_far,
    first_ref,
    second_ref,
    sums,
    result,
    landed,
    local_sems,
    edge_sems,
    ready,
    in_send,
    in_recv,
    out_send,
    out_recv,
):
    hi, lo, cut = lax.axis_index("hi"), lax.axis_index("lo"), lax.axis_index("cuts")
    other = 1 - cut
    span_hi, span_lo = GATE // count_hi, GATE // count_lo
    half = count_hi // 2
    upper, inner = hi // half, hi % half
    rows = GATE // 2
    per = span_hi // 2
    blocks = count_hi * count_lo
    turns = edges_ref.shape[0]
    edges = gate_ref.shape[0]
    near = [(a, b) for a in range(half) for b in range(count_lo)]
    cores = [(a, b, core) for a, b in near for core in range(CLOSED)]

    def keeper(a, b, core):
        if core == CLOSED - 1 and a == half - 1:
            return 0
        if core == CLOSED - 1 and b == 1:
            return 1
        return None

    def holder(a, core, half_index):
        return a

    def here(a, b, core):
        return (inner == holder(a, core, upper)) & (lo == b) & (cut == core)

    def any_of(half_index):
        return functools.reduce(
            lambda p, q: p | q,
            [here(*spot) for spot in cores if keeper(*spot) == half_index],
            hi < 0,
        )

    kept = [any_of(0), any_of(1)]
    wide_role = (kept[0] & (upper == 0)) | (kept[1] & (upper == 1))
    idle = (kept[0] & (upper == 1)) | (kept[1] & (upper == 0))
    slots = []
    for spot in cores:
        done = sum(keeper(*item) is None for item in cores[: len(slots)])
        slots.append((len(slots), len(cores) + done))
    mine = [0, 0]
    for spot, pair in zip(cores, slots):
        for side in range(2):
            index = pair[side if keeper(*spot) is None else 0]
            mine[side] += here(*spot).astype(jnp.int32) * index
    taken = len(cores) + sum(keeper(*spot) is None for spot in cores)
    pairs = (
        (x_hbm, x_ref),
        (edges_hbm, edges_ref),
        (orders_hbm, orders_ref),
        (closing_hbm, closing_ref),
        (gate_hbm, gate_ref),
    )
    gets = [pltpu.make_async_copy(*pair, local_sems.at[i]) for i, pair in enumerate(pairs)]
    for get in gets:
        get.start()

    def device(side, a, b, core):
        th = flipped(upper, side) * half + flipped(inner, a)
        return {"hi": th, "lo": flipped(lo, b), "cuts": core}

    def greet(semaphore, side):
        for a, b in near:
            for core in range(CLOSED):
                if side or a or b:
                    pl.semaphore_signal(
                        semaphore, inc=1, device_id=device(side, a, b, core), device_id_type=MESH
                    )

    barrier = pltpu.get_barrier_semaphore()
    pl.semaphore_signal(barrier, inc=1, device_id={"cuts": other}, device_id_type=MESH)
    greet(barrier, 0)

    @pl.when((upper == 0) | kept[1])
    def _():
        greet(barrier, 1)

    gets[0].wait()
    stride = count_hi * CLOSED * count_lo
    for b in range(count_hi):
        for e in range(count_lo):
            start = b * CLOSED * count_lo + cut * count_lo + e
            outgoing[b * count_lo + e] = x_ref[pl.ds(start, span_hi, stride=stride), :]
    guests = sum(keeper(*spot) == 1 for spot in cores)
    pl.semaphore_wait(barrier, blocks - 1 + jnp.where(upper == 1, blocks, guests))

    for half_index, order in enumerate(ORDERS):
        for group in order:
            for a, b, core in cores:
                keep = keeper(a, b, core)
                kind = "S" if keep is None else "W" if keep == half_index else "F"
                if kind != group:
                    continue
                goal_half = half_index if keep is None else keep
                goal = holder(a, core, goal_half)
                k = (inner ^ goal) + (half if kind == "F" else 0)
                copy = pltpu.make_async_remote_copy(
                    src_ref=outgoing.at[(a * CLOSED + core) * count_lo + b],
                    dst_ref=arrived.at[k, lo ^ b, cut],
                    send_sem=in_send,
                    recv_sem=in_recv.at[k],
                    device_id={"hi": goal + goal_half * half, "lo": b, "cuts": core},
                    device_id_type=MESH,
                )
                away = upper == half_index
                if kind != "F":
                    away = away & ~here(a, b, core)
                pl.when(away)(copy.start)
    own = holder(inner, cut, upper)
    own_copy = pltpu.make_async_copy(
        outgoing.at[(own * CLOSED + cut) * count_lo + lo], arrived.at[0, 0, cut], in_recv.at[0]
    )
    pl.when(~idle)(own_copy.start)

    gets[1].wait()
    edge_copy = pltpu.make_async_remote_copy(
        src_ref=edges_ref,
        dst_ref=edges_far,
        send_sem=edge_sems.at[0],
        recv_sem=edge_sems.at[1],
        device_id={"cuts": other},
        device_id_type=MESH,
    )
    edge_copy.start()

    @pl.when(upper == 1)
    def _():
        greet(ready, 1)

    gets[2].wait()
    down = lax.broadcasted_iota(jnp.int32, (GATE, GATE), 0)
    along = lax.broadcasted_iota(jnp.int32, (GATE, GATE), 1)

    def high_bits(side, a):
        return (side ^ upper) * half + (a ^ inner)

    column = down % span_hi * count_hi + high_bits(down // rows, down % rows // span_hi)
    columns = (column == along).astype(FULL).astype(HALF)
    rows_one = (source_row(column, orders_ref, 0) == along).astype(FULL).astype(HALF)
    row = (down // span_lo ^ lo) * span_lo + down % span_lo
    rows_two = (source_row(row, orders_ref, 1) == along).astype(FULL).astype(HALF)

    gets[3].wait()
    gets[4].wait()
    edge_copy.wait()
    wide = CLOSED * span_hi

    def pick(s, place, values):
        chosen = edges_ref if s < turns else edges_far
        turn = s % turns
        total = None
        for c in range(edges):
            weight = (chosen[turn : turn + 1, place : place + 1] == c).astype(FULL)
            term = weight * values(c)
            total = term if total is None else total + term
        return total

    def build_first(s, far):
        fronts = pick(s, 2, lambda c: closing_ref[c, 0])
        gate = pick(s, 0, lambda c: gate_ref[c])
        split = [halves(gate * fronts[z : z + 1]) for z in range(CLOSED)]
        chosen_rows = rows_one[far * rows : (far + 1) * rows]
        for part in range(2):
            moved = [dot(chosen_rows, split[z][part]).astype(HALF) for z in range(CLOSED)]
            moved = dot(columns, jnp.concatenate(moved, axis=0), ((1,), (1,))).astype(HALF)
            for side in range(2):
                for a in range(half):
                    for z in range(CLOSED):
                        start = z * rows + a * span_hi
                        first_ref[
                            far * half + a,
                            side,
                            part * rows : (part + 1) * rows,
                            s * wide + z * span_hi : s * wide + (z + 1) * span_hi,
                        ] = moved[side * rows : (side + 1) * rows, start : start + span_hi]

    rears = []
    for s in range(2 * turns):
        rears.append(pick(s, 2, lambda c: closing_ref[c, 1]))
        build_first(s, 0)
        for part, piece in enumerate(halves(pick(s, 1, lambda c: gate_ref[c]))):
            second_ref[part, s] = dot(rows_two, piece).astype(HALF)

    @pl.when(wide_role)
    def _():
        for s in range(2 * turns):
            build_first(s, 1)

    def advance(a):
        pltpu.make_async_copy(arrived.at[a], arrived.at[a], in_recv.at[a]).wait()
        piece = jnp.concatenate(
            [arrived[a, b].reshape(wide, span_lo) for b in range(count_lo)], axis=1
        )
        high, low = halves(piece)
        pair = jnp.concatenate([high, low], axis=0)
        parts = []
        for s in range(2 * turns):
            both = dot(pair, second_ref[0, s])
            part = both[:wide] + both[wide:] + dot(high, second_ref[1, s])
            for z in range(CLOSED):
                parts.append(part[z * span_hi : (z + 1) * span_hi] * rears[s][z : z + 1])
        high, low = halves(jnp.concatenate(parts, axis=0))

        def side_sum(side):
            both = dot(first_ref[a, side], high)
            return both[:rows] + both[rows:] + dot(first_ref[a, side, :rows, :], low)

        return side_sum

    def gather(a, start=False):
        side_sum = advance(a)
        for side in range(2):
            if start:
                sums[side] = side_sum(side)
            else:
                sums[side] += side_sum(side)

    outs = []
    for goal in range(2):
        side = goal ^ upper
        for a, b, core in cores if goal == 0 else sorted(cores, key=lambda spot: (-spot[0], -spot[1])):
            source = result.at[
                goal, b, pl.ds(pl.multiple_of((inner ^ a) * span_hi + core * per, per), per)
            ]
            target = landed.at[jnp.where(side == 0, mine[0], mine[1])]
            copy = pltpu.make_async_remote_copy(
                src_ref=source,
                dst_ref=target,
                send_sem=out_send,
                recv_sem=out_recv,
                device_id={"hi": goal * half + a, "lo": b, "cuts": core},
                device_id_type=MESH,
            )
            at_home = (upper == goal) & (inner == a) & (lo == b) & (cut == core)
            outs.append((goal, ~at_home, copy))

    def finish(a):
        side_sum = advance(a)
        for goal in range(2):
            side = goal ^ upper
            total = sums[side] + side_sum(side)
            for e in range(count_lo):
                result[goal, e] = total[:, e * span_lo : (e + 1) * span_lo]
            if goal:

                @pl.when(upper == 0)
                def _():
                    pl.semaphore_wait(ready, blocks)

            for order, away, copy in outs:
                if order == goal:
                    pl.when(away)(copy.start)
        pltpu.make_async_copy(
            result.at[upper, lo, pl.ds(pl.multiple_of((cut * per), per), per)],
            landed.at[mine[0]],
            out_recv,
        ).start()

    @pl.when(~wide_role & ~idle)
    def _():
        for a in range(half - 1):
            gather(a, a == 0)
        finish(half - 1)

    @pl.when(kept[0] & (upper == 0))
    def _():
        for a in STEPS[0][:-1]:
            gather(a, a == STEPS[0][0])
        finish(STEPS[0][-1])

    @pl.when(kept[1] & (upper == 1))
    def _():
        for a in STEPS[1][:-1]:
            gather(a, a == STEPS[1][0])
        finish(STEPS[1][-1])

    @pl.when(idle & (upper == 0))
    def _():
        pl.semaphore_wait(ready, blocks)

    arrivals = landed.at[pl.ds(0, taken)]

    pltpu.make_async_copy(arrivals, arrivals, out_recv).wait()
    for (a, b, core), (first, second) in zip(cores, slots):
        place = pl.ds((a * CLOSED + core) * count_lo + b, per, stride=blocks)
        if keeper(a, b, core) is not None:
            out_ref[place, :] = landed[first]
        else:
            out_ref[place, :] = landed[first] + landed[second]
    gone = outgoing.at[pl.ds(0, blocks - 1)]
    pltpu.make_async_copy(gone, gone, in_send).wait()

    @pl.when(idle)
    def _():
        pltpu.make_async_copy(outgoing.at[0], outgoing.at[0], in_send).wait()

    @pl.when(~idle)
    def _():
        gone = landed.at[pl.ds(0, 2 * blocks - 1)]
        pltpu.make_async_copy(gone, gone, out_send).wait()


def local(state_block, gate_table, closing_table, slice_edges, bit_orders):
    count_hi = lax.axis_size("hi")
    count_lo = lax.axis_size("lo")
    span_hi = GATE // count_hi
    span_lo = GATE // count_lo
    blocks = count_hi * count_lo
    half = count_hi // 2
    middle = state_block.shape[2] // (GATE * GATE * CLOSED)
    fits = middle == 1 and span_lo == 128 and span_hi % 16 == 0 and count_hi == len(STEPS[0])
    if not fits or lax.axis_size("cuts") != CLOSED:
        return local_plain(state_block, gate_table, closing_table, slice_edges, bit_orders)
    slices = slice_edges.shape[0] * CLOSED
    rows = GATE // 2
    per = span_hi // 2
    hbm = pl.BlockSpec(memory_space=pltpu.HBM)
    dma = pltpu.SemaphoreType.DMA
    out = pl.pallas_call(
        functools.partial(kernel, count_hi, count_lo),
        out_shape=jax.ShapeDtypeStruct((per * blocks, span_lo), FULL),
        in_specs=[hbm] * 5,
        out_specs=pl.BlockSpec(memory_space=pltpu.VMEM),
        scratch_shapes=[
            pltpu.VMEM((span_hi * blocks * CLOSED, span_lo), FULL),
            pltpu.VMEM(gate_table.shape, FULL),
            pltpu.VMEM(closing_table.shape, FULL),
            pltpu.VMEM(slice_edges.shape, jnp.int32),
            pltpu.SMEM(bit_orders.shape, jnp.int32),
            pltpu.VMEM((blocks, span_hi, span_lo), FULL),
            pltpu.VMEM((count_hi, count_lo, CLOSED, span_hi, span_lo), FULL),
            pltpu.VMEM(slice_edges.shape, jnp.int32),
            pltpu.VMEM((count_hi, 2, 2 * rows, slices * CLOSED * span_hi), HALF),
            pltpu.VMEM((2, slices, GATE, GATE), HALF),
            pltpu.VMEM((2, rows, GATE), FULL),
            pltpu.VMEM((2, count_lo, rows, span_lo), FULL),
            pltpu.VMEM((2 * blocks, per, span_lo), FULL),
            dma((5,)),
            dma((2,)),
            pltpu.SemaphoreType.REGULAR,
            dma(()),
            dma((count_hi,)),
            dma(()),
            dma(()),
        ],
        compiler_params=pltpu.CompilerParams(
            collective_id=0, has_side_effects=True, vmem_limit_bytes=32 * 1024 * 1024
        ),
    )(
        *(
            pltpu.with_memory_space_constraint(item, pltpu.HBM)
            for item in (
                state_block.reshape(-1, span_lo),
                gate_table,
                closing_table,
                slice_edges,
                bit_orders,
            )
        )
    )
    return out.reshape(1, 1, -1)


def solution(mesh):
    in_specs = (P(("group", "hi"), "lo", None), P(), P(), P(("group", "cuts"), None), P())
    out_specs = P(("group", "hi"), "lo", "cuts")
    return jax.shard_map(local, mesh=mesh, in_specs=in_specs, out_specs=out_specs, check_vma=False)
```

```python
import functools

import jax
import jax.numpy as jnp
from jax import lax
from jax.experimental import pallas as pl
from jax.experimental.pallas import tpu as pltpu
from jax.sharding import PartitionSpec as P

BITS = 8
STEPS = ((3, 0, 1, 2), (3, 0, 2, 1))
ORDERS = ("SFW", "SFW")
GATE = 256
CLOSED = 2


def permuted(gate, order):
    rows = jnp.arange(GATE, dtype=jnp.int32)
    picked = rows[:, None] >> order[None, :] & 1
    weights = jnp.left_shift(jnp.ones((BITS,), jnp.int32), jnp.arange(BITS, dtype=jnp.int32))
    source = jnp.sum(picked * weights[None, :], axis=1)
    return jnp.take(gate, source, axis=0)


def local_plain(state_block, gate_table, closing_table, slice_edges, bit_orders):
    count_hi = lax.axis_size("hi")
    count_lo = lax.axis_size("lo")
    span_hi = GATE // count_hi
    span_lo = GATE // count_lo
    middle = state_block.shape[2] // (GATE * GATE * CLOSED)
    tensor = state_block.reshape(span_hi, count_hi, CLOSED, middle, count_lo, span_lo)
    turns = slice_edges.shape[0]
    firsts = []
    seconds = []
    fronts = []
    rears = []
    for turn_index in range(turns):
        chosen = slice_edges[turn_index]
        firsts.append(permuted(gate_table[chosen[0]], bit_orders[0]))
        seconds.append(permuted(gate_table[chosen[1]], bit_orders[1]))
        fronts.append(closing_table[chosen[2], 0])
        rears.append(closing_table[chosen[2], 1])
    section_ones = []
    for turn_index in range(turns):

        def apply_first(piece, first=firsts[turn_index], front=fronts[turn_index]):
            shape = piece.shape
            flat = piece.reshape(GATE, -1)
            product = lax.dot_general(
                first,
                flat,
                (((0,), (0,)), ((), ())),
                precision=lax.Precision.HIGHEST,
                preferred_element_type=jnp.float32,
            )
            scaled = jnp.transpose(front).reshape(shape[0], shape[1], shape[2], 1, 1, 1)
            return product.reshape(shape) * scaled

        section_ones.append(
            apply_first(lax.all_to_all(tensor, "hi", split_axis=1, concat_axis=1, tiled=True))
        )
    total = jnp.zeros((span_hi, count_hi, middle, count_lo, span_lo), jnp.float32)
    for turn_index in range(turns):
        current = section_ones[turn_index]

        def apply_second(piece, second=seconds[turn_index], rear=rears[turn_index]):
            shape = piece.shape
            flat = piece.reshape(-1, GATE)
            product = jnp.dot(
                flat, second, precision=lax.Precision.HIGHEST, preferred_element_type=jnp.float32
            )
            product = product.reshape(shape[0], shape[1], shape[2], shape[3], GATE)
            closed = jnp.einsum("phzkg,zg->phkg", product, rear, precision=lax.Precision.HIGHEST)
            return closed.reshape(shape[0], shape[1], shape[3], shape[4], shape[5])

        total = total + apply_second(
            lax.all_to_all(current, "lo", split_axis=4, concat_axis=4, tiled=True)
        )
    placed = lax.all_to_all(
        lax.all_to_all(total, "hi", split_axis=1, concat_axis=1, tiled=True),
        "lo",
        split_axis=3,
        concat_axis=3,
        tiled=True,
    )
    summed = lax.psum_scatter(placed.reshape(-1), "cuts", scatter_dimension=0, tiled=True)
    return summed.reshape(1, 1, -1)


MESH = pl.DeviceIdType.MESH
HALF = jnp.bfloat16
FULL = jnp.float32


def dot(left, right, dims=((1,), (0,))):
    return lax.dot_general(left, right, (dims, ((), ())), preferred_element_type=FULL)


def halves(value):
    high = value.astype(HALF)
    return high, (value - high.astype(FULL)).astype(HALF)


def source_row(index, orders_ref, section):
    total = jnp.zeros_like(index)
    for bit in range(BITS):
        picked = lax.shift_right_logical(index, jnp.full_like(index, orders_ref[section, bit])) & 1
        total = total | (picked << bit)
    return total


def flipped(index, mask):
    bit = 1
    while bit <= mask:
        if mask & bit:
            index = index + bit - 2 * bit * (index // bit % 2)
        bit *= 2
    return index


def kernel(
    count_hi,
    count_lo,
    x_hbm,
    gate_hbm,
    closing_hbm,
    edges_hbm,
    orders_hbm,
    out_ref,
    x_ref,
    gate_ref,
    closing_ref,
    edges_ref,
    orders_ref,
    outgoing,
    arrived,
    edges_far,
    first_ref,
    second_ref,
    sums,
    result,
    landed,
    local_sems,
    edge_sems,
    ready,
    in_send,
    in_recv,
    out_send,
    out_recv,
):
    hi, lo, cut = lax.axis_index("hi"), lax.axis_index("lo"), lax.axis_index("cuts")
    other = 1 - cut
    span_hi, span_lo = GATE // count_hi, GATE // count_lo
    half = count_hi // 2
    upper, inner = hi // half, hi % half
    rows = GATE // 2
    per = span_hi // 2
    blocks = count_hi * count_lo
    turns = edges_ref.shape[0]
    edges = gate_ref.shape[0]
    near = [(a, b) for a in range(half) for b in range(count_lo)]
    cores = [(a, b, core) for a, b in near for core in range(CLOSED)]

    def keeper(a, b, core):
        if core == CLOSED - 1 and a == half - 1:
            return 0
        if core == CLOSED - 1 and b == 1:
            return 1
        return None

    def holder(a, core, half_index):
        return a

    def here(a, b, core):
        return (inner == holder(a, core, upper)) & (lo == b) & (cut == core)

    def any_of(half_index):
        return functools.reduce(
            lambda p, q: p | q,
            [here(*spot) for spot in cores if keeper(*spot) == half_index],
            hi < 0,
        )

    kept = [any_of(0), any_of(1)]
    wide_role = (kept[0] & (upper == 0)) | (kept[1] & (upper == 1))
    idle = (kept[0] & (upper == 1)) | (kept[1] & (upper == 0))
    slots = []
    for spot in cores:
        done = sum(keeper(*item) is None for item in cores[: len(slots)])
        slots.append((len(slots), len(cores) + done))
    mine = [0, 0]
    for spot, pair in zip(cores, slots):
        for side in range(2):
            index = pair[side if keeper(*spot) is None else 0]
            mine[side] += here(*spot).astype(jnp.int32) * index
    taken = len(cores) + sum(keeper(*spot) is None for spot in cores)
    pairs = (
        (x_hbm, x_ref),
        (edges_hbm, edges_ref),
        (orders_hbm, orders_ref),
        (closing_hbm, closing_ref),
        (gate_hbm, gate_ref),
    )
    gets = [pltpu.make_async_copy(*pair, local_sems.at[i]) for i, pair in enumerate(pairs)]
    for get in gets:
        get.start()

    def device(side, a, b, core):
        th = flipped(upper, side) * half + flipped(inner, a)
        return {"hi": th, "lo": flipped(lo, b), "cuts": core}

    def greet(semaphore, side):
        for a, b in near:
            for core in range(CLOSED):
                if side or a or b:
                    pl.semaphore_signal(
                        semaphore, inc=1, device_id=device(side, a, b, core), device_id_type=MESH
                    )

    barrier = pltpu.get_barrier_semaphore()
    pl.semaphore_signal(barrier, inc=1, device_id={"cuts": other}, device_id_type=MESH)
    greet(barrier, 0)

    @pl.when((upper == 0) | kept[1])
    def _():
        greet(barrier, 1)

    gets[0].wait()
    stride = count_hi * CLOSED * count_lo
    for b in range(count_hi):
        for e in range(count_lo):
            start = b * CLOSED * count_lo + cut * count_lo + e
            outgoing[b * count_lo + e] = x_ref[pl.ds(start, span_hi, stride=stride), :]
    guests = sum(keeper(*spot) == 1 for spot in cores)
    pl.semaphore_wait(barrier, blocks - 1 + jnp.where(upper == 1, blocks, guests))

    for half_index, order in enumerate(ORDERS):
        for group in order:
            for a, b, core in cores:
                keep = keeper(a, b, core)
                kind = "S" if keep is None else "W" if keep == half_index else "F"
                if kind != group:
                    continue
                goal_half = half_index if keep is None else keep
                goal = holder(a, core, goal_half)
                k = (inner ^ goal) + (half if kind == "F" else 0)
                copy = pltpu.make_async_remote_copy(
                    src_ref=outgoing.at[(a * CLOSED + core) * count_lo + b],
                    dst_ref=arrived.at[k, lo ^ b, cut],
                    send_sem=in_send,
                    recv_sem=in_recv.at[k],
                    device_id={"hi": goal + goal_half * half, "lo": b, "cuts": core},
                    device_id_type=MESH,
                )
                away = upper == half_index
                if kind != "F":
                    away = away & ~here(a, b, core)
                pl.when(away)(copy.start)
    own = holder(inner, cut, upper)
    own_copy = pltpu.make_async_copy(
        outgoing.at[(own * CLOSED + cut) * count_lo + lo], arrived.at[0, 0, cut], in_recv.at[0]
    )
    pl.when(~idle)(own_copy.start)

    gets[1].wait()
    edge_copy = pltpu.make_async_remote_copy(
        src_ref=edges_ref,
        dst_ref=edges_far,
        send_sem=edge_sems.at[0],
        recv_sem=edge_sems.at[1],
        device_id={"cuts": other},
        device_id_type=MESH,
    )
    edge_copy.start()

    @pl.when(upper == 1)
    def _():
        greet(ready, 1)

    gets[2].wait()
    down = lax.broadcasted_iota(jnp.int32, (GATE, GATE), 0)
    along = lax.broadcasted_iota(jnp.int32, (GATE, GATE), 1)

    def high_bits(side, a):
        return (side ^ upper) * half + (a ^ inner)

    column = down % span_hi * count_hi + high_bits(down // rows, down % rows // span_hi)
    columns = (column == along).astype(FULL).astype(HALF)
    rows_one = (source_row(column, orders_ref, 0) == along).astype(FULL).astype(HALF)
    row = (down // span_lo ^ lo) * span_lo + down % span_lo
    rows_two = (source_row(row, orders_ref, 1) == along).astype(FULL).astype(HALF)

    gets[3].wait()
    gets[4].wait()
    edge_copy.wait()
    wide = CLOSED * span_hi

    def pick(s, place, values):
        chosen = edges_ref if s < turns else edges_far
        turn = s % turns
        total = None
        for c in range(edges):
            weight = (chosen[turn : turn + 1, place : place + 1] == c).astype(FULL)
            term = weight * values(c)
            total = term if total is None else total + term
        return total

    def build_first(s, far):
        fronts = pick(s, 2, lambda c: closing_ref[c, 0])
        gate = pick(s, 0, lambda c: gate_ref[c])
        split = [halves(gate * fronts[z : z + 1]) for z in range(CLOSED)]
        chosen_rows = rows_one[far * rows : (far + 1) * rows]
        for part in range(2):
            moved = [dot(chosen_rows, split[z][part]).astype(HALF) for z in range(CLOSED)]
            moved = dot(columns, jnp.concatenate(moved, axis=0), ((1,), (1,))).astype(HALF)
            for side in range(2):
                for a in range(half):
                    for z in range(CLOSED):
                        start = z * rows + a * span_hi
                        first_ref[
                            far * half + a,
                            side,
                            part * rows : (part + 1) * rows,
                            s * wide + z * span_hi : s * wide + (z + 1) * span_hi,
                        ] = moved[side * rows : (side + 1) * rows, start : start + span_hi]

    rears = []
    for s in range(2 * turns):
        rears.append(pick(s, 2, lambda c: closing_ref[c, 1]))
        build_first(s, 0)
        for part, piece in enumerate(halves(pick(s, 1, lambda c: gate_ref[c]))):
            second_ref[part, s] = dot(rows_two, piece).astype(HALF)

    @pl.when(wide_role)
    def _():
        for s in range(2 * turns):
            build_first(s, 1)

    def advance(a):
        pltpu.make_async_copy(arrived.at[a], arrived.at[a], in_recv.at[a]).wait()
        piece = jnp.concatenate(
            [arrived[a, b].reshape(wide, span_lo) for b in range(count_lo)], axis=1
        )
        high, low = halves(piece)
        pair = jnp.concatenate([high, low], axis=0)
        parts = []
        for s in range(2 * turns):
            both = dot(pair, second_ref[0, s])
            part = both[:wide] + both[wide:] + dot(high, second_ref[1, s])
            for z in range(CLOSED):
                parts.append(part[z * span_hi : (z + 1) * span_hi] * rears[s][z : z + 1])
        high, low = halves(jnp.concatenate(parts, axis=0))

        def side_sum(side):
            both = dot(first_ref[a, side], high)
            return both[:rows] + both[rows:] + dot(first_ref[a, side, :rows, :], low)

        return side_sum

    def gather(a, start=False):
        side_sum = advance(a)
        for side in range(2):
            if start:
                sums[side] = side_sum(side)
            else:
                sums[side] += side_sum(side)

    outs = []
    for goal in range(2):
        side = goal ^ upper
        for a, b, core in cores if goal == 0 else sorted(cores, key=lambda spot: (-spot[0], -spot[1])):
            source = result.at[
                goal, b, pl.ds(pl.multiple_of((inner ^ a) * span_hi + core * per, per), per)
            ]
            target = landed.at[jnp.where(side == 0, mine[0], mine[1])]
            copy = pltpu.make_async_remote_copy(
                src_ref=source,
                dst_ref=target,
                send_sem=out_send,
                recv_sem=out_recv,
                device_id={"hi": goal * half + a, "lo": b, "cuts": core},
                device_id_type=MESH,
            )
            at_home = (upper == goal) & (inner == a) & (lo == b) & (cut == core)
            outs.append((goal, ~at_home, copy))

    def finish(a):
        side_sum = advance(a)
        for goal in range(2):
            side = goal ^ upper
            total = sums[side] + side_sum(side)
            for e in range(count_lo):
                result[goal, e] = total[:, e * span_lo : (e + 1) * span_lo]
            if goal:

                @pl.when(upper == 0)
                def _():
                    pl.semaphore_wait(ready, blocks)

            for order, away, copy in outs:
                if order == goal:
                    pl.when(away)(copy.start)
        pltpu.make_async_copy(
            result.at[upper, lo, pl.ds(pl.multiple_of((cut * per), per), per)],
            landed.at[mine[0]],
            out_recv,
        ).start()

    @pl.when(~wide_role & ~idle)
    def _():
        for a in range(half - 1):
            gather(a, a == 0)
        finish(half - 1)

    @pl.when(kept[0] & (upper == 0))
    def _():
        for a in STEPS[0][:-1]:
            gather(a, a == STEPS[0][0])
        finish(STEPS[0][-1])

    @pl.when(kept[1] & (upper == 1))
    def _():
        for a in STEPS[1][:-1]:
            gather(a, a == STEPS[1][0])
        finish(STEPS[1][-1])

    @pl.when(idle & (upper == 0))
    def _():
        pl.semaphore_wait(ready, blocks)

    arrivals = landed.at[pl.ds(0, taken)]

    pltpu.make_async_copy(arrivals, arrivals, out_recv).wait()
    for (a, b, core), (first, second) in zip(cores, slots):
        place = pl.ds((a * CLOSED + core) * count_lo + b, per, stride=blocks)
        if keeper(a, b, core) is not None:
            out_ref[place, :] = landed[first]
        else:
            out_ref[place, :] = landed[first] + landed[second]
    gone = outgoing.at[pl.ds(0, blocks - 1)]
    pltpu.make_async_copy(gone, gone, in_send).wait()

    @pl.when(idle)
    def _():
        pltpu.make_async_copy(outgoing.at[0], outgoing.at[0], in_send).wait()

    @pl.when(~idle)
    def _():
        gone = landed.at[pl.ds(0, 2 * blocks - 1)]
        pltpu.make_async_copy(gone, gone, out_send).wait()


def local(state_block, gate_table, closing_table, slice_edges, bit_orders):
    count_hi = lax.axis_size("hi")
    count_lo = lax.axis_size("lo")
    span_hi = GATE // count_hi
    span_lo = GATE // count_lo
    blocks = count_hi * count_lo
    half = count_hi // 2
    middle = state_block.shape[2] // (GATE * GATE * CLOSED)
    fits = middle == 1 and span_lo == 128 and span_hi % 16 == 0 and count_hi == len(STEPS[0])
    if not fits or lax.axis_size("cuts") != CLOSED:
        return local_plain(state_block, gate_table, closing_table, slice_edges, bit_orders)
    slices = slice_edges.shape[0] * CLOSED
    rows = GATE // 2
    per = span_hi // 2
    hbm = pl.BlockSpec(memory_space=pltpu.HBM)
    dma = pltpu.SemaphoreType.DMA
    out = pl.pallas_call(
        functools.partial(kernel, count_hi, count_lo),
        out_shape=jax.ShapeDtypeStruct((per * blocks, span_lo), FULL),
        in_specs=[hbm] * 5,
        out_specs=pl.BlockSpec(memory_space=pltpu.VMEM),
        scratch_shapes=[
            pltpu.VMEM((span_hi * blocks * CLOSED, span_lo), FULL),
            pltpu.VMEM(gate_table.shape, FULL),
            pltpu.VMEM(closing_table.shape, FULL),
            pltpu.VMEM(slice_edges.shape, jnp.int32),
            pltpu.SMEM(bit_orders.shape, jnp.int32),
            pltpu.VMEM((blocks, span_hi, span_lo), FULL),
            pltpu.VMEM((count_hi, count_lo, CLOSED, span_hi, span_lo), FULL),
            pltpu.VMEM(slice_edges.shape, jnp.int32),
            pltpu.VMEM((count_hi, 2, 2 * rows, slices * CLOSED * span_hi), HALF),
            pltpu.VMEM((2, slices, GATE, GATE), HALF),
            pltpu.VMEM((2, rows, GATE), FULL),
            pltpu.VMEM((2, count_lo, rows, span_lo), FULL),
            pltpu.VMEM((2 * blocks, per, span_lo), FULL),
            dma((5,)),
            dma((2,)),
            pltpu.SemaphoreType.REGULAR,
            dma(()),
            dma((count_hi,)),
            dma(()),
            dma(()),
        ],
        compiler_params=pltpu.CompilerParams(
            collective_id=0, has_side_effects=True, vmem_limit_bytes=32 * 1024 * 1024
        ),
    )(
        *(
            pltpu.with_memory_space_constraint(item, pltpu.HBM)
            for item in (
                state_block.reshape(-1, span_lo),
                gate_table,
                closing_table,
                slice_edges,
                bit_orders,
            )
        )
    )
    return out.reshape(1, 1, -1)


def solution(mesh):
    in_specs = (P(("group", "hi"), "lo", None), P(), P(), P(("group", "cuts"), None), P())
    out_specs = P(("group", "hi"), "lo", "cuts")
    return jax.shard_map(local, mesh=mesh, in_specs=in_specs, out_specs=out_specs, check_vma=False)
```
